256 devices in a mesh: grp: 2 (over z), kvp: 16 (over x, core), tp: 8 (over y).
Axes of the slice: x: 8, y: 8, z: 2, core: 2. Of those that a mesh axis runs over, the one named last changes fastest.
The devices are a block of a 8x8x16 slice.
Arguments:
- hidden_in: bfloat16 [16, 7168], P('grp'), parts along dimension 0, may hold values from -3 to 3
- queries_nope: bfloat16 [16, 128, 128], P('grp', ('kvp', 'tp')), parts along dimension 0, may hold values from -6 to 6
- queries_rope: bfloat16 [16, 128, 64], P('grp', ('kvp', 'tp')), parts along dimension 0, may hold values from -26 to 26
- cache: bfloat16 [16, 6144, 576], P('grp', 'kvp'), parts along dimension 0, may hold values from -20 to 20
- lengths: int32 [16], P('grp'), parts along dimension 0, may hold values from 128 to 6144, as said below
- w_uk: bfloat16 [128, 128, 512], P(('kvp', 'tp')), may hold values from -0.5 to 0.5
- w_uv: bfloat16 [128, 512, 128], P(('kvp', 'tp')), may hold values from -0.25 to 0.25
- w_out: bfloat16 [16384, 7168], P(('kvp', 'tp')), may hold values from -0.1875 to 0.1875
- norm_gain: float32 [7168], replicated, may hold values from 0.25 to 1.75
- w_gate: bfloat16 [7168, 18432], P(None, ('kvp', 'tp')), may hold values from -0.0625 to 0.0625
- w_up: bfloat16 [7168, 18432], P(None, ('kvp', 'tp')), may hold values from -0.0625 to 0.0625
- w_down: bfloat16 [18432, 7168], P(('kvp', 'tp')), may hold values from -0.15625 to 0.15625
Outputs:
- layer_out: bfloat16 [16, 7168], P('grp', ('kvp', 'tp')), parts along dimension 0
The draws below stay inside these ranges and needn't reach their ends.
There are 2 independent parts, one for each index of `grp`. The reference program is written for one: setup_inputs(seed, part) draws one part's arguments, and reference() takes and returns one part's arrays. A program takes and returns all parts, laid end to end along the dimension named above; an argument that names none is the same for every part. Nothing has to cross between parts.
Inputs may be any that keep to these rules, and one draw needn't show every extreme that they name: `lengths`: every length is a multiple of 128; in every draw some request has the full 6144.
All inputs are finite; a program needn't handle non-finite values.
Results may differ from the reference program's by a relative error of at most 0.04.
Values may be sent and summed in bfloat16 or wider, within the bound.
No kernel may reach another device: no remote copies, remote signals or barrier semaphores. Data moves between devices by JAX's collectives and lax.ppermute only.
A program may use at most 64 MiB of HBM per device.

```python
import jax
import jax.numpy as jnp
from jax import lax

D = 7168
FF = 18432
H = 128
LAT = 512
ROPE = 64
HEAD_DIM = 128
BATCH = 8
BLOCK = 128
CTX_DEV = 384
CTX = 6144
N_KVP = 16


def draw_lengths(key, part):
    count_blocks = CTX // BLOCK
    counts = jax.random.randint(key, (BATCH,), 1, count_blocks + 1)
    full_row = jax.random.randint(jax.random.fold_in(key, 3), (), 0, BATCH)
    counts = jnp.where(jnp.arange(BATCH) == full_row, count_blocks, counts)
    return (counts * BLOCK).astype(jnp.int32)


def draw_cache(key, part):
    values = jnp.clip(jax.random.normal(jax.random.fold_in(key, 11), (BATCH, CTX, LAT + ROPE), jnp.float32), -6.0, 6.0)
    return values.astype(jnp.bfloat16)


def draw_queries_rope(key, part):
    values = jnp.clip(jax.random.normal(jax.random.fold_in(key, 21), (BATCH, H, ROPE), jnp.float32), -6.0, 6.0)
    return values.astype(jnp.bfloat16)


def strengthened(drawn, key, source, target, shards_of, factor):
    def block_of(position):
        return (jnp.arange(drawn.shape[position]) // (drawn.shape[position] // shards_of)).reshape((-1,) + (1,) * (drawn.ndim - 1 - position))

    first = jax.random.permutation(key, shards_of)[block_of(target)]
    far = (block_of(target) + shards_of // 2) % shards_of
    return jnp.where((block_of(source) == first) | (block_of(source) == far), factor * drawn, drawn)


def block_scale(own_key, shape, pieces, smallest, largest):
    level = 1.0
    for position, shards_of in pieces:
        heights = jax.random.uniform(jax.random.fold_in(jax.random.fold_in(own_key, 6), position), (shards_of,), jnp.float32, smallest / len(pieces), largest / len(pieces))
        level = level * jnp.repeat(jnp.exp(heights), shape[position] // shards_of).reshape((-1,) + (1,) * (len(shape) - 1 - position))
    return level


def centred(own_key, extent, scale, most, shards=(), kind=jnp.bfloat16):
    result = jax.random.normal(own_key, extent, jnp.float32) * scale
    if len(shards) > 0:
        result = block_scale(own_key, extent, shards, -0.22, 0.18) * result
    return jnp.clip(result, min=-most, max=most).astype(kind)


def heavy_noise(own_key, extent, deviation, bound, cuts, heavy, kind=jnp.bfloat16):
    entries = deviation * jax.random.normal(own_key, extent, jnp.float32)
    if cuts:
        entries = entries * block_scale(own_key, extent, cuts, -0.22, 0.18)
    return jnp.clip(strengthened(entries, jax.random.fold_in(own_key, 3), *heavy), -bound, bound).astype(kind)


def setup_inputs(seed: int = 0, part: int = 0) -> dict:
    key_of = jax.random.split(jax.random.key(seed), 13)
    own_keys = jax.random.split(jax.random.fold_in(key_of[12], part), 13)
    hidden_in = centred(own_keys[0], (BATCH, D), 0.5, 3.0)
    queries_nope = centred(own_keys[1], (BATCH, H, HEAD_DIM), 1.0, 6.0, ((1, 128),))
    queries_rope = draw_queries_rope(jax.random.fold_in(jax.random.fold_in(key_of[12], part), 71), part)
    cache = draw_cache(jax.random.fold_in(jax.random.fold_in(key_of[12], part), 71), part)
    lengths = draw_lengths(jax.random.fold_in(jax.random.fold_in(key_of[12], part), 71), part)
    w_uk = centred(key_of[5], (H, HEAD_DIM, LAT), HEAD_DIM ** -0.5, 0.5, ((0, 128),))
    w_uv = centred(key_of[6], (H, LAT, HEAD_DIM), LAT ** -0.5, 0.25, ((0, 128),))
    w_out = heavy_noise(key_of[7], (H * HEAD_DIM, D), (H * HEAD_DIM) ** -0.5, 0.1875, ((0, 128),), (0, 1, 128, 5.5))
    norm_gain = jnp.clip(1.0 + 0.15 * jax.random.normal(key_of[8], (D,), jnp.float32), 0.25, 1.75)
    w_gate = centred(key_of[9], (D, FF), D ** -0.5, 0.0625, ((1, 128),))
    w_up = centred(key_of[10], (D, FF), D ** -0.5, 0.0625, ((1, 128),))
    w_down = heavy_noise(key_of[11], (FF, D), FF ** -0.5, 0.15625, ((0, 128),), (0, 1, 128, 5.5))
    return {"hidden_in": hidden_in, "queries_nope": queries_nope, "queries_rope": queries_rope, "cache": cache, "lengths": lengths, "w_uk": w_uk, "w_uv": w_uv, "w_out": w_out, "norm_gain": norm_gain, "w_gate": w_gate, "w_up": w_up, "w_down": w_down}


def reference(hidden_in, queries_nope, queries_rope, cache, lengths, w_uk, w_uv, w_out, norm_gain, w_gate, w_up, w_down):
    score_scale = float(HEAD_DIM + ROPE) ** (-0.5)
    q_lat = jnp.einsum('bhd,hdl->bhl', queries_nope.astype(jnp.float32), w_uk.astype(jnp.float32)).astype(jnp.bfloat16)
    q_full = jnp.concatenate([q_lat, queries_rope], axis=2).astype(jnp.float32)
    cache_wide = cache.astype(jnp.float32)
    scores = jnp.einsum('bhc,btc->bht', q_full, cache_wide) * score_scale
    visible = jnp.arange(CTX, dtype=jnp.int32)[None, :] < lengths[:, None]
    visible = jnp.broadcast_to(visible[:, None, :], scores.shape).reshape(BATCH, H, N_KVP, CTX_DEV)
    blocks = scores.reshape(BATCH, H, N_KVP, CTX_DEV)
    masked = jnp.where(visible, blocks, jnp.float32(-1e+30))
    block_max = lax.optimization_barrier(jnp.max(masked, axis=3))
    exponent = jnp.where(visible, jnp.exp(masked - block_max[..., None]), jnp.float32(0.0))
    block_sum = lax.optimization_barrier(jnp.sum(exponent, axis=3))
    guarded = jnp.maximum(block_sum, 1.0)
    log_total = block_max + jnp.log(guarded)
    weights = (exponent / guarded[..., None]).astype(jnp.bfloat16)
    cache_blocks = cache_wide.reshape(BATCH, N_KVP, CTX_DEV, LAT + ROPE)
    partial_value = jnp.einsum('bhkt,bktc->bhkc', weights.astype(jnp.float32), cache_blocks)[..., :LAT]
    highest = lax.optimization_barrier(jnp.max(log_total, axis=2))
    overall = highest + jnp.log(lax.optimization_barrier(jnp.sum(jnp.exp(log_total - highest[..., None]), axis=2)))
    o_lat = lax.optimization_barrier(jnp.sum(jnp.exp(log_total - overall[..., None])[..., None] * partial_value, axis=2)).astype(jnp.bfloat16)
    head_out = jnp.einsum('bhl,hle->bhe', o_lat.astype(jnp.float32), w_uv.astype(jnp.float32)).astype(jnp.bfloat16)
    attention = jnp.dot(head_out.reshape(BATCH, H * HEAD_DIM), w_out, preferred_element_type=jnp.float32)
    residual = hidden_in.astype(jnp.float32) + attention
    mean_square = lax.optimization_barrier(jnp.mean(residual * residual, axis=1))
    normed = (residual * lax.rsqrt(mean_square + 1e-06)[:, None] * norm_gain.astype(jnp.float32)[None, :]).astype(jnp.bfloat16)
    gate_proj = jnp.dot(normed, w_gate, preferred_element_type=jnp.float32)
    up_proj = jnp.dot(normed, w_up, preferred_element_type=jnp.float32)
    act = (jax.nn.silu(gate_proj) * up_proj).astype(jnp.bfloat16)
    ffn_out = jnp.dot(act, w_down, preferred_element_type=jnp.float32)
    return (residual + ffn_out).astype(jnp.bfloat16)
```

```python
import jax
import jax.numpy as jnp
from jax import lax
from jax.sharding import Mesh
from jax.sharding import PartitionSpec as P

KVP = ("kvp_0", "kvp_1")
KVP_TP = ("kvp_0", "kvp_1", "tp")
F32 = jnp.float32
BF16 = jnp.bfloat16


def exchange(blocks, axes):
    return lax.all_to_all(blocks, axes, split_axis=0, concat_axis=0, tiled=True)


def spread(value, axes):
    return exchange(jnp.broadcast_to(value[None], (lax.axis_size(axes), *value.shape)), axes)


def in_blocks(value, size):
    rows, width = value.shape
    return jnp.moveaxis(value.reshape(rows, size, width // size), 1, 0)


def per_device(
    hidden_in,
    queries_nope,
    queries_rope,
    cache,
    lengths,
    w_uk,
    w_uv,
    w_out,
    norm_gain,
    w_gate,
    w_up,
    w_down,
):
    batch, heads_dev, head_dim = queries_nope.shape
    latent = w_uk.shape[2]
    ctx_dev = cache.shape[1]
    groups = lax.axis_size(KVP)
    columns = lax.axis_size("tp")
    score_scale = float(head_dim + queries_rope.shape[2]) ** (-0.5)
    q_lat = jnp.dot(queries_nope[:, 0], w_uk[0], preferred_element_type=F32).astype(BF16)
    q_full = spread(jnp.concatenate([q_lat, queries_rope[:, 0]], axis=1), KVP)
    scores = jnp.einsum("hbc,btc->bht", q_full, cache, preferred_element_type=F32) * score_scale
    offset = lax.axis_index(KVP) * ctx_dev
    visible = ((offset + jnp.arange(ctx_dev, dtype=jnp.int32))[None, :] < lengths[:, None])[
        :, None, :
    ]
    masked = jnp.where(visible, scores, F32(-1e30))
    block_max = jnp.max(masked, axis=2)
    exponent = jnp.where(visible, jnp.exp(masked - block_max[..., None]), F32(0.0))
    guarded = jnp.maximum(jnp.sum(exponent, axis=2), 1.0)
    log_total = block_max + jnp.log(guarded)
    weights = (exponent / guarded[..., None]).astype(BF16)
    partial_value = jnp.einsum("bht,btc->hbc", weights, cache, preferred_element_type=F32)[
        ..., :latent
    ]
    logs = log_total.T[..., None]
    high = lax.reduce_precision(logs, 8, 7)
    low = logs - high
    lane = lax.broadcasted_iota(jnp.int32, (1, 1, 128), 2)
    tail = jnp.where(lane == 0, high, jnp.where(lane == 1, low, F32(0.0)))
    parts = exchange(jnp.concatenate([partial_value, tail], axis=2).astype(BF16), KVP)
    part_logs = parts[..., latent].astype(F32) + parts[..., latent + 1].astype(F32)
    highest = jnp.max(part_logs, axis=0)
    overall = highest + jnp.log(jnp.sum(jnp.exp(part_logs - highest[None]), axis=0))
    share = jnp.exp(part_logs - overall[None])[..., None]
    o_lat = jnp.sum(share * parts[..., :latent].astype(F32), axis=0).astype(BF16)
    head_out = jnp.dot(o_lat, w_uv[0], preferred_element_type=F32).astype(BF16)
    attention = jnp.dot(head_out, w_out, preferred_element_type=F32).astype(BF16)

    slab = jnp.sum(exchange(in_blocks(attention, groups), KVP).astype(F32), axis=0)
    slab = jnp.sum(spread(slab.astype(BF16), "tp").astype(F32), axis=0)
    slab_width = slab.shape[1]
    share_width = slab_width // columns
    hidden_slab = lax.dynamic_slice_in_dim(
        hidden_in, lax.axis_index(KVP) * slab_width, slab_width, 1
    )
    slab = slab + hidden_slab.astype(F32)
    residual_share = lax.dynamic_slice_in_dim(
        slab, lax.axis_index("tp") * share_width, share_width, 1
    )
    residual = jnp.moveaxis(spread(slab.astype(BF16), KVP), 0, 1).reshape(batch, -1).astype(F32)
    mean_square = jnp.mean(residual * residual, axis=1)
    normed = (residual * lax.rsqrt(mean_square + 1e-06)[:, None] * norm_gain[None, :]).astype(BF16)
    gate_proj = jnp.dot(normed, w_gate, preferred_element_type=F32)
    up_proj = jnp.dot(normed, w_up, preferred_element_type=F32)
    act = (jax.nn.silu(gate_proj) * up_proj).astype(BF16)
    ffn_terms = jnp.dot(act, w_down, preferred_element_type=F32).astype(BF16)
    ffn_blocks = exchange(in_blocks(ffn_terms, groups * columns), KVP_TP)
    ffn_share = jnp.sum(ffn_blocks.astype(F32), axis=0)
    return (residual_share + ffn_share).astype(BF16)


def solution(mesh):
    torus = Mesh(
        mesh.devices.reshape(
            mesh.shape["grp"], mesh.shape["kvp"] // 2, 2, mesh.shape["tp"]
        ),
        ("grp", "kvp_0", "kvp_1", "tp"),
    )
    return jax.shard_map(
        per_device,
        mesh=torus,
        in_specs=(
            P("grp", None),
            P("grp", KVP_TP, None),
            P("grp", KVP_TP, None),
            P("grp", KVP, None),
            P("grp"),
            P(KVP_TP, None, None),
            P(KVP_TP, None, None),
            P(KVP_TP, None),
            P(),
            P(None, KVP_TP),
            P(None, KVP_TP),
            P(KVP_TP, None),
        ),
        out_specs=P("grp", KVP_TP),
        check_vma=False,
    )
```

```python
import functools

import jax
import jax.numpy as jnp
from jax import lax
from jax.experimental import pallas as pl
from jax.experimental.pallas import tpu as pltpu
from jax.sharding import Mesh
from jax.sharding import PartitionSpec as P

KVP = ("kvp_0", "kvp_1")
KVP_TP = ("kvp_0", "kvp_1", "tp")
F32 = jnp.float32
BF16 = jnp.bfloat16
LANES = 128
OUT_CHUNKS = 4
OUT_GRANT = 3 << 20
FFN_GRANT = 8 << 20
VMEM = pl.BlockSpec(memory_space=pltpu.VMEM)
HBM = pl.BlockSpec(memory_space=pltpu.HBM)


def exchange(blocks, axes):
    return lax.all_to_all(blocks, axes, split_axis=0, concat_axis=0, tiled=True)


def call(body, outs, specs, *operands, scratch=(), grant=2 << 20):
    return pl.pallas_call(
        body,
        out_shape=outs,
        in_specs=specs,
        out_specs=[VMEM] * len(outs),
        scratch_shapes=scratch,
        compiler_params=pltpu.CompilerParams(vmem_limit_bytes=grant),
    )(*operands)


def stay(array):
    return pltpu.with_memory_space_constraint(array, pltpu.HBM)


def columns_of(source, target, sems, first, count):
    width = source.shape[1] // count
    copies = []
    for i in range(count):
        part = (slice(None), pl.ds(i * width, width))
        copies.append(
            pltpu.make_async_copy(source.at[part], target.at[part], sems.at[first + i])
        )
    return copies


def query_kernel(nope, rope, w_uk, out):
    q_lat = jnp.dot(nope[...], w_uk[...], preferred_element_type=F32).astype(BF16)
    latent = q_lat.shape[1]
    for k in range(out.shape[0]):
        out[k, :, :latent] = q_lat
        out[k, :, latent:] = rope[...]


def project_kernel(parts, w_uv, w_out, out, value, rows, sems):
    groups, batch, width = parts.shape
    latent = width - LANES
    first = pltpu.make_async_copy(w_uv, value, sems.at[0])
    chunks = columns_of(w_out, rows, sems, 1, OUT_CHUNKS)
    for copy in (first, *chunks):
        copy.start()
    tail = parts[:, :, latent:].astype(F32)
    logs = tail + pltpu.roll(tail, LANES // 2, 2)
    highest = jnp.max(logs, axis=0)
    overall = highest + jnp.log(jnp.sum(jnp.exp(logs - highest[None]), axis=0))
    share = jnp.exp(logs - overall[None])
    pieces = []
    for at in range(0, latent, LANES):
        piece = jnp.sum(share * parts[:, :, at : at + LANES].astype(F32), axis=0)
        pieces.append(piece.astype(BF16))
    o_lat = jnp.concatenate(pieces, axis=1)
    first.wait()
    head_out = jnp.dot(o_lat, value[...], preferred_element_type=F32).astype(BF16)
    block = out.shape[2]
    for k in range(0, groups, 2):
        if k % (groups // OUT_CHUNKS) == 0:
            chunks[k // (groups // OUT_CHUNKS)].wait()
        both = jnp.dot(
            head_out, rows[:, k * block : (k + 2) * block], preferred_element_type=F32
        )
        out[k] = both[:, :block].astype(BF16)
        out[k + 1] = both[:, block:].astype(BF16)


def sum_kernel(blocks, out):
    total = jnp.sum(blocks[...].astype(F32), axis=0).astype(BF16)
    for t in range(out.shape[0]):
        out[t] = total


def residual_kernel(blocks, hidden, gain, out, slab):
    batch, block = hidden.shape
    total = jnp.sum(blocks[...].astype(F32), axis=0) + hidden[...]
    slab[...] = total
    square = jnp.sum(total * total, axis=1, keepdims=True)
    high = square.astype(BF16).astype(F32)
    spare = out.shape[2] - block
    lane = lax.broadcasted_iota(jnp.int32, (batch, spare), 1)
    tail = jnp.where(lane < spare // 2, high, square - high)
    message = jnp.concatenate([total * gain[...], tail], axis=1).astype(BF16)
    for j in range(out.shape[0]):
        out[j] = message


def ffn_kernel(blocks, gate, up, down, out, value, gates, ups, downs, sems):
    groups, batch, padded = blocks.shape
    width = gate.shape[1]
    block = width // groups
    spare = padded - block
    gate_in = columns_of(gate, gates, sems, 0, 2)
    up_in = columns_of(up, ups, sems, 2, 2)
    down_in = columns_of(down, downs, sems, 4, 2)
    for copy in (gate_in[0], up_in[0], gate_in[1], up_in[1], down_in[0], down_in[1]):
        copy.start()
    tail = jnp.sum(blocks[:, :, padded - LANES :].astype(F32), axis=0)
    square = (
        tail[:, LANES - spare : LANES - spare + 1]
        + tail[:, LANES - spare // 2 : LANES - spare // 2 + 1]
    )
    scale = lax.rsqrt(square / width + 1e-06)
    for k in range(0, groups, 2):
        both = jnp.concatenate(
            [blocks[k].astype(F32)[:, :block], blocks[k + 1].astype(F32)[:, :block]], axis=1
        )
        value[:, k * block : (k + 2) * block] = both.astype(BF16)
    contract = (((1,), (1,)), ((), ()))
    gate_proj = jnp.zeros((batch, gate.shape[0]), F32)
    up_proj = jnp.zeros((batch, gate.shape[0]), F32)
    for i in range(2):
        half = slice(i * (width // 2), (i + 1) * (width // 2))
        gate_in[i].wait()
        gate_proj += lax.dot_general(
            value[:, half], gates[:, half], contract, preferred_element_type=F32
        )
        up_in[i].wait()
        up_proj += lax.dot_general(
            value[:, half], ups[:, half], contract, preferred_element_type=F32
        )
    gate_proj = gate_proj * scale
    up_proj = up_proj * scale
    act = (gate_proj / (1.0 + jnp.exp(-gate_proj)) * up_proj).astype(BF16)
    pieces = out.shape[0] // groups
    share = block // pieces
    fill = jnp.zeros((batch // 2, LANES - 2 * share), F32)
    for k in range(0, groups, 2):
        if k % (groups // 2) == 0:
            down_in[k // (groups // 2)].wait()
        at = k * block
        both = jnp.dot(act, downs[:, at : at + 2 * block], preferred_element_type=F32)
        for j in range(2 * pieces):
            piece = both[:, j * share : (j + 1) * share]
            packed = jnp.concatenate([piece[: batch // 2], piece[batch // 2 :], fill], axis=1)
            out[k * pieces + j] = packed.astype(BF16)


def final_kernel(blocks, slab, out):
    batch, share = out.shape
    total = jnp.sum(blocks[...].astype(F32), axis=0)
    total = jnp.concatenate([total[:, :share], total[:, share : 2 * share]], axis=0)
    t_here = lax.axis_index("tp")
    own = jnp.zeros((batch, share), F32)
    for t in range(slab.shape[1] // share):
        own = jnp.where(t_here == t, slab[:, t * share : (t + 1) * share], own)
    out[...] = (total + own).astype(BF16)


def per_device(
    hidden_in,
    queries_nope,
    queries_rope,
    cache,
    lengths,
    w_uk,
    w_uv,
    w_out,
    norm_gain,
    w_gate,
    w_up,
    w_down,
):
    batch, heads_dev, head_dim = queries_nope.shape
    latent = w_uk.shape[2]
    rope_dim = queries_rope.shape[2]
    ctx_dev = cache.shape[1]
    model_width = norm_gain.shape[0]
    groups = lax.axis_size(KVP)
    columns = lax.axis_size("tp")
    block = model_width // groups
    share_width = block // columns
    padded = -(-block // LANES) * LANES
    shape = jax.ShapeDtypeStruct
    score_scale = float(head_dim + rope_dim) ** (-0.5)

    (q_blocks,) = call(
        query_kernel,
        [shape((groups, batch, latent + rope_dim), BF16)],
        [VMEM] * 3,
        queries_nope[:, 0],
        queries_rope[:, 0],
        w_uk[0],
        grant=60 << 20,
    )
    q_full = exchange(q_blocks, KVP)
    offset = lax.axis_index(KVP) * ctx_dev
    visible = (offset + jnp.arange(ctx_dev, dtype=jnp.int32))[None, :] < lengths[:, None]
    start = lax.axis_index(KVP) * block
    hidden_slab = lax.dynamic_slice_in_dim(hidden_in, start, block, 1).astype(F32)
    gain_slab = lax.dynamic_slice_in_dim(norm_gain, start, block, 0)
    gain_slab = jnp.broadcast_to(gain_slab[None], hidden_slab.shape)
    visible, hidden_slab, gain_slab = lax.optimization_barrier((visible, hidden_slab, gain_slab))
    visible = visible[:, None, :]
    scores = jnp.einsum("hbc,btc->bht", q_full, cache, preferred_element_type=F32) * score_scale
    masked = jnp.where(visible, scores, F32(-1e30))
    block_max = jnp.max(masked, axis=2)
    exponent = jnp.where(visible, jnp.exp(masked - block_max[..., None]), F32(0.0))
    guarded = jnp.maximum(jnp.sum(exponent, axis=2), 1.0)
    log_total = block_max + jnp.log(guarded)
    weights = (exponent / guarded[..., None]).astype(BF16)
    partial_value = jnp.einsum("bht,btc->hbc", weights, cache, preferred_element_type=F32)[
        ..., :latent
    ]
    logs = log_total.T[..., None]
    high = lax.reduce_precision(logs, 8, 7)
    low = logs - high
    lane = lax.broadcasted_iota(jnp.int32, (1, 1, LANES), 2)
    tail = jnp.where(lane < LANES // 2, high, low)
    parts = exchange(jnp.concatenate([partial_value, tail], axis=2).astype(BF16), KVP)

    (terms,) = call(
        project_kernel,
        [shape((groups, batch, block), BF16)],
        [VMEM, HBM, HBM],
        parts,
        stay(w_uv[0]),
        stay(w_out),
        scratch=[
            pltpu.VMEM(w_uv.shape[1:], BF16),
            pltpu.VMEM(w_out.shape, BF16),
            pltpu.SemaphoreType.DMA((1 + OUT_CHUNKS,)),
        ],
        grant=OUT_GRANT,
    )
    terms = exchange(terms, KVP)
    (sums,) = call(sum_kernel, [shape((columns, batch, block), BF16)], [VMEM], terms)
    sums = exchange(sums, "tp")
    residual, slab = call(
        residual_kernel,
        [shape((groups, batch, padded), BF16), shape((batch, block), F32)],
        [VMEM, VMEM, VMEM],
        sums,
        hidden_slab,
        gain_slab,
    )
    residual = exchange(residual, KVP)
    hidden_dev = w_gate.shape[1]
    (ffn_terms,) = call(
        ffn_kernel,
        [shape((groups * columns, batch // 2, LANES), BF16)],
        [VMEM, HBM, HBM, HBM],
        residual,
        stay(w_gate.T),
        stay(w_up.T),
        stay(w_down),
        scratch=[
            pltpu.VMEM((batch, model_width), BF16),
            pltpu.VMEM((hidden_dev, model_width), BF16),
            pltpu.VMEM((hidden_dev, model_width), BF16),
            pltpu.VMEM((hidden_dev, model_width), BF16),
            pltpu.SemaphoreType.DMA((6,)),
        ],
        grant=FFN_GRANT,
    )
    ffn_terms = exchange(ffn_terms, KVP_TP)
    (out,) = call(
        final_kernel, [shape((batch, share_width), BF16)], [VMEM, VMEM], ffn_terms, slab
    )
    return out


def solution(mesh):
    torus = Mesh(
        mesh.devices.reshape(mesh.shape["grp"], mesh.shape["kvp"] // 2, 2, mesh.shape["tp"]),
        ("grp", "kvp_0", "kvp_1", "tp"),
    )
    return jax.shard_map(
        per_device,
        mesh=torus,
        in_specs=(
            P("grp", None),
            P("grp", KVP_TP, None),
            P("grp", KVP_TP, None),
            P("grp", KVP, None),
            P("grp"),
            P(KVP_TP, None, None),
            P(KVP_TP, None, None),
            P(KVP_TP, None),
            P(),
            P(None, KVP_TP),
            P(None, KVP_TP),
            P(KVP_TP, None),
        ),
        out_specs=P("grp", KVP_TP),
        check_vma=False,
    )
```
